256 devices in a mesh: row: 32 (over y, x, core), col: 8 (over z).
Axes of the slice: x: 4, y: 4, z: 8, core: 2. Of those that a mesh axis runs over, the one named last changes fastest.
Arguments:
- item_factors: bfloat16 [32768, 128], P(('row', 'col')), may hold values from -0.5 to 0.5
- item_index: int32 [2048, 8192], P('col', 'row'), may hold values from 0 to 1023
- ratings: bfloat16 [2048, 8192], P('col', 'row'), may hold values from -4 to 4
- counts: int32 [2048, 32], P('col', 'row'), may hold values from 1 to 256, as said below
Outputs:
- user_factors: float32 [8, 256, 128], P('col', 'row')
The draws below stay inside these ranges and needn't reach their ends.
Inputs may be any that keep to these rules, and one draw needn't show every extreme that they name: `counts`: for each user block and item block, some user has exactly 256 live slots.
All inputs are finite; a program needn't handle non-finite values.
Results may differ from the reference program's by a relative error of at most 0.0004.
Values may be sent and summed in bfloat16 or wider, within the bound.
No kernel may reach another device: no remote copies, remote signals or barrier semaphores. Data moves between devices by JAX's collectives and lax.ppermute only.
A program may use at most 192 MiB of HBM per device.

```python
import jax
import jax.numpy as jnp
from jax import lax

RANK = 128
SLOTS = 256
ITEM_DEV = 128
USERS = 2048
ITEMS = 32768
N_ROW = 32
N_COL = 8


def draw_counts(key, part):
    first, second, third, fourth = jax.random.split(jax.random.fold_in(key, 11), 4)
    tile = jnp.arange(N_ROW, dtype=jnp.int32)
    ceiling = SLOTS // 4 + 3 * SLOTS // 4 * tile // max(N_ROW - 1, 1)
    level = jax.random.randint(fourth, (USERS, 1), 0, 8)
    shift_by = jnp.where(level < 5, 0, 2 * (level - 4)).astype(jnp.int32)
    reach = jnp.maximum(jnp.right_shift(ceiling[None, :], shift_by), 1)
    raw_bits = jax.random.randint(first, (USERS, N_ROW), 0, 1 << 20)
    value = 1 + raw_bits % reach
    heavy = jax.random.randint(second, (USERS, 1), 1, 3)
    value = jnp.minimum(value * heavy, SLOTS)
    user_block = USERS // N_COL
    picked = jax.random.randint(third, (N_COL, N_ROW), 0, user_block)
    within = jnp.arange(USERS, dtype=jnp.int32) % user_block
    block_id = jnp.arange(USERS, dtype=jnp.int32) // user_block
    forced = within[:, None] == picked[block_id]
    return jnp.where(forced, SLOTS, value).astype(jnp.int32)


def set_ends(entries, rng, least, top_value):
    dims = entries.shape
    index_at = [jax.random.randint(jax.random.fold_in(rng, axis), (), 0, dims[axis]) for axis in range(len(dims))]
    entries = entries.at[tuple(index_at)].set(least)
    longest = dims.index(max(dims))
    index_at[longest] = (index_at[longest] + 1) % dims[longest]
    return entries.at[tuple(index_at)].set(top_value)


def block_scale(stream_key, dims, cuts, least, high):
    factor_of, own = 1.0, jax.random.fold_in(stream_key, 6)
    for dim, parts in cuts:
        draws = jnp.exp(jax.random.uniform(jax.random.fold_in(own, dim), (parts,), jnp.float32, least / len(cuts), high / len(cuts)))
        factor_of = factor_of * jnp.repeat(draws, dims[dim] // parts).reshape([-1 if axis == dim else 1 for axis in range(len(dims))])
    return factor_of


def scatter_about(rng, dims, width, limit, pieces=(), kind=jnp.bfloat16):
    values = width * jax.random.normal(rng, dims, jnp.float32)
    if pieces:
        values = values * block_scale(rng, dims, pieces, -0.22, 0.18)
    return jnp.clip(values, -limit, limit).astype(kind)


def setup_inputs(seed: int = 0) -> dict:
    streams_of = jax.random.split(jax.random.key(seed), 5)
    item_factors = scatter_about(streams_of[0], (ITEMS, RANK), RANK ** -0.5, 0.5, ((0, 256),))
    item_index = set_ends(jax.random.randint(streams_of[1], (USERS, N_ROW * SLOTS), 0, N_COL * ITEM_DEV), jax.random.fold_in(streams_of[1], 1), 0, (N_COL * ITEM_DEV) - 1).astype(jnp.int32)
    ratings = scatter_about(streams_of[2], (USERS, N_ROW * SLOTS), 1.0, 4.0, ((0, 8), (1, 32)))
    counts = draw_counts(jax.random.fold_in(streams_of[4], 71), 0)
    return dict(item_factors=item_factors, item_index=item_index, ratings=ratings, counts=counts)


def solve_users(normal_sum, right_side, number):
    width_rank = normal_sum.shape[-1]
    shifted = normal_sum + (0.1 * number / width_rank)[:, None, None] * jnp.eye(width_rank, dtype=jnp.float32)
    factor_low = jnp.linalg.cholesky(shifted)
    middle = jax.scipy.linalg.solve_triangular(factor_low, right_side[:, :, None], lower=True)
    answer = jax.scipy.linalg.solve_triangular(factor_low, middle, lower=True, trans=1)
    return answer[:, :, 0]

def reference(item_factors, item_index, ratings, counts):
    tile_width = N_COL * ITEM_DEV
    slot_tile = jnp.arange(N_ROW * SLOTS, dtype=jnp.int32) // SLOTS
    slot_place = jnp.arange(N_ROW * SLOTS, dtype=jnp.int32) % SLOTS
    global_index = (item_index + (slot_tile * tile_width)[None, :]).astype(jnp.int32)
    live_slot = (slot_place[None, :] < jnp.repeat(counts, SLOTS, axis=1)).astype(jnp.bfloat16)
    groups = USERS // N_ROW

    def one_group(packed):
        index_rows, rating_rows, live_rows = packed
        chosen = jnp.take(item_factors, index_rows, axis=0)
        weighted = (chosen * live_rows[:, :, None]).astype(jnp.float32)
        scaled = (rating_rows * live_rows).astype(jnp.float32)
        normal_sum = jnp.einsum('usa,usb->uab', weighted, weighted, precision=lax.Precision.HIGHEST)
        right_side = jnp.einsum('us,usa->ua', scaled, weighted, precision=lax.Precision.HIGHEST)
        return (normal_sum, right_side)
    normal_sum, right_side = lax.map(one_group, (global_index.reshape(groups, N_ROW, -1), ratings.reshape(groups, N_ROW, -1), live_slot.reshape(groups, N_ROW, -1)))
    normal_sum = normal_sum.reshape(USERS, RANK, RANK)
    right_side = right_side.reshape(USERS, RANK)
    number = jnp.sum(counts.astype(jnp.float32), axis=1)
    answer = solve_users(normal_sum, right_side, number)
    return answer.reshape(N_COL, USERS // N_COL, RANK)
```

```python
import functools

import jax
import jax.numpy as jnp
from jax import lax
from jax.experimental import pallas as pl
from jax.experimental.pallas import tpu as pltpu
from jax.sharding import PartitionSpec as P

F32, BF16 = jnp.float32, jnp.bfloat16
LOW = 256
PANEL = 8
ROWS_TO_ROWS = (((1,), (1,)), ((), ()))


def gram_kernel(code_ref, table_ref, gram_ref, code_s, rows_s, *, slots, rank):
    users = code_s.shape[0]
    shards = table_ref.shape[1]
    per = LOW // table_ref.shape[3]
    parts = shards // per

    @pl.when(pl.program_id(0) == 0)
    def _():
        gram_ref[...] = jnp.zeros(gram_ref.shape, F32)

    code_s[...] = code_ref[0].astype(F32)
    table = jnp.concatenate(
        [jnp.concatenate([table_ref[0, per * h + q] for q in range(per)], axis=1) for h in range(parts)], axis=0
    )
    row_ids = lax.broadcasted_iota(jnp.int32, (LOW, slots), 0).astype(F32).astype(BF16)
    one, zero = jnp.ones((), BF16), jnp.zeros((), BF16)
    for u in range(users):
        row = code_s[u : u + 1, :]
        low = jnp.broadcast_to(row[:, :slots], (16, slots)).astype(BF16)
        low = jnp.concatenate([low] * (LOW // 16), axis=0)
        found = jnp.dot(table, jnp.where(row_ids == low, one, zero), preferred_element_type=F32)
        high = jnp.broadcast_to(row[:, slots : 2 * slots], (rank, slots))
        rows = jnp.zeros((rank, slots), F32)
        for h in range(parts):
            rows = jnp.where(high == h, found[h * rank : (h + 1) * rank], rows)
        rows_s[u, :rank] = rows.astype(BF16)
        rows_s[u, rank:] = jnp.broadcast_to(row[:, 2 * slots :], (16, slots)).astype(BF16)
    for u in range(users):
        both = rows_s[u]
        out = lax.dot_general(both, both[:rank], ROWS_TO_ROWS, preferred_element_type=F32)
        gram_ref[u] += out[: rank + 8]


def gram(code, table, slots):
    blocks, users, _ = code.shape
    _, shards, rank, items = table.shape
    return pl.pallas_call(
        functools.partial(gram_kernel, slots=slots, rank=rank),
        grid=(blocks,),
        in_specs=[
            pl.BlockSpec((1, users, 3 * slots), lambda k: (k, 0, 0)),
            pl.BlockSpec((1, shards, rank, items), lambda k: (k, 0, 0, 0)),
        ],
        out_specs=pl.BlockSpec((users, rank + 8, rank), lambda k: (0, 0, 0)),
        out_shape=jax.ShapeDtypeStruct((users, rank + 8, rank), F32),
        scratch_shapes=[pltpu.VMEM((users, 3 * slots), F32), pltpu.VMEM((users, rank + 16, slots), BF16)],
        name="gram",
    )(code, table)


def solve_kernel(gram_ref, number_ref, out_ref, rows_s):
    users, rank = out_ref.shape
    lane = lax.broadcasted_iota(jnp.int32, (users, rank), 1)
    shift = 0.1 * number_ref[...] / rank
    for i in range(rank):
        row = gram_ref[:, i, :]
        rows_s[i] = jnp.where(lane == i, row + shift, row)
    right = gram_ref[:, rank, :]

    def lane_of(value, i):
        return jnp.broadcast_to(value[:, i : i + 1], (users, rank))

    answer = jnp.zeros((users, rank), F32)
    for start in range(0, rank, PANEL):
        steps = range(PANEL)
        rows = [rows_s[start + t] for t in steps]
        corner = {(t, s): lane_of(rows[s], start + t) for t in steps for s in range(t + 1)}
        middle = [lane_of(right, start + t) for t in steps]
        inside = (lane >= start) & (lane < start + PANEL)
        rows = [jnp.where(inside, jnp.where(lane == start + t, 1.0, 0.0), rows[t]) for t in steps]
        inverse = []
        for s in steps:
            inverse.append(1.0 / corner[s, s])
            for t in range(s + 1, PANEL):
                factor = corner[t, s] * inverse[s]
                for q in range(s + 1, t + 1):
                    corner[t, q] = corner[t, q] - factor * corner[q, s]
                rows[t] = rows[t] - factor * rows[s]
                middle[t] = middle[t] - factor * middle[s]
        for t in steps:
            scaled = middle[t] * inverse[t]
            answer = answer + jnp.where(lane < start + PANEL, scaled * rows[t], 0.0)
            right = right - scaled * rows[t]
        below = [rows[t] * inverse[t] for t in steps]
        for i in range(start + PANEL, rank):
            row = jnp.where(inside, 0.0, rows_s[i])
            for t in steps:
                row = row - lane_of(below[t], i) * rows[t]
            rows_s[i] = row
    out_ref[...] = answer


def solve(gram_sum, number):
    users, rank = number.shape
    return pl.pallas_call(
        solve_kernel,
        out_shape=jax.ShapeDtypeStruct((users, rank), F32),
        scratch_shapes=[pltpu.VMEM((rank, users, rank), F32)],
        name="solve",
    )(gram_sum, number)


def coded(item_index, ratings, counts):
    position = lax.broadcasted_iota(jnp.int32, item_index.shape, 1)
    dead = LOW
    high = jnp.where(position < counts, item_index // LOW, dead)
    return jnp.concatenate([(item_index % LOW).astype(BF16), high.astype(BF16), ratings], axis=1)


def per_device(item_factors, item_index, ratings, counts):
    slots, rank = item_index.shape[1], item_factors.shape[1]
    n_row, n_col = lax.axis_size("row"), lax.axis_size("col")
    code = coded(item_index, ratings, counts).reshape(n_row, -1, 3 * slots)
    code = lax.all_to_all(code, "row", 0, 0, tiled=True)
    table = lax.all_gather(lax.optimization_barrier(item_factors.T), ("row", "col"))
    table = table.reshape(n_row, n_col, rank, -1)
    number = jnp.sum((code[:, :, slots : 2 * slots] < LOW).astype(F32), axis=(0, 2))
    number = jnp.broadcast_to(number[:, None], (number.shape[0], rank))
    return solve(gram(code, table, slots), number)[None]


def solution(mesh):
    return jax.shard_map(
        per_device,
        mesh=mesh,
        in_specs=(P(("row", "col"), None), P("col", "row"), P("col", "row"), P("col", "row")),
        out_specs=P("col", "row", None),
        check_vma=False,
    )
```

```python
import functools

import jax
import jax.numpy as jnp
import numpy as np
from jax import lax
from jax.experimental import pallas as pl
from jax.experimental.pallas import tpu as pltpu
from jax.sharding import PartitionSpec as P


F32, BF16 = jnp.float32, jnp.bfloat16
LOW = 256
HALF = 128
SIDE = 4
CORES = 2
PANEL = 8
ROWS_TO_ROWS = (((1,), (1,)), ((), ()))


def gram_kernel(source_ref, code_ref, *refs, counts, first, offset):
    tables = refs[: len(counts)]
    before = refs[len(counts) : -8]
    own_ref, other_ref, table_s, low_s, high_s, rate_s, live_s, rows_s = refs[-8:]
    sums = (own_ref, other_ref)
    users, slots = low_s.shape
    rank = own_ref.shape[2]
    step = pl.program_id(0)

    @pl.when(step == 0)
    def _():
        for n, sum_ref in enumerate(sums):
            sum_ref[...] = jnp.zeros(sum_ref.shape, F32) if first else before[n][...]

    begin = 0
    for table_ref, count in zip(tables, counts):

        @pl.when((step >= begin) & (step < begin + count))
        def _(table_ref=table_ref, begin=begin):
            per = LOW // table_ref.shape[3]
            for z in range(table_ref.shape[1]):
                h, q = z // per, z % per
                table_s[h * rank : (h + 1) * rank, q * 128 : (q + 1) * 128] = table_ref[step - begin, z]

        begin += count

    code = code_ref[source_ref[offset + step]].astype(F32)
    index = code[:, :slots]
    size = jnp.abs(index)
    above = [jnp.where(size >= LOW * 2**e, 1.0, 0.0) for e in range(3)]
    low_s[...] = index * (1.0 - 0.5 * above[0] - 0.25 * above[1] - 0.125 * above[2])
    high_s[...] = above[0] + above[1] + above[2]
    rate_s[...] = code[:, slots:]
    live = jnp.where(size > 0.0, 1.0, 0.0)
    live_s[...] = live[:, : slots // 2] + live[:, slots // 2 :]

    place = lax.broadcasted_iota(jnp.int32, (LOW, slots), 0)
    row_ids = jnp.where(place < HALF, place + HALF, -place).astype(F32).astype(BF16)
    one, zero = jnp.ones((), BF16), jnp.zeros((), BF16)
    table = table_s[...]
    parts = table.shape[0] // rank
    for u in range(users):
        low = jnp.broadcast_to(low_s[u : u + 1], (16, slots)).astype(BF16)
        low = jnp.concatenate([low] * (LOW // 16), axis=0)
        found = jnp.dot(table, jnp.where(row_ids == low, one, zero), preferred_element_type=F32)
        high = jnp.broadcast_to(high_s[u : u + 1], (rank, slots))
        rows = found[:rank]
        for h in range(1, parts):
            rows = jnp.where(high == h, found[h * rank : (h + 1) * rank], rows)
        rows_s[u, :rank] = rows.astype(BF16)
        rows_s[u, rank:] = jnp.broadcast_to(rate_s[u : u + 1], (16, slots)).astype(BF16)
    tail_row = lax.broadcasted_iota(jnp.int32, (8, rank), 0)
    for u in range(users):
        both = rows_s[u]
        out = lax.dot_general(both, both[:rank], ROWS_TO_ROWS, preferred_element_type=F32)
        sum_ref, v = sums[u // (users // CORES)], u % (users // CORES)
        sum_ref[v, :rank] += out[:rank]
        tail = jnp.where(tail_row == 1, jnp.broadcast_to(live_s[u : u + 1], (8, rank)), out[rank : rank + 8])
        sum_ref[v, rank:] += tail


def gram(source, offset, code, tables, before=()):
    _, users, width = code.shape
    slots = width // 2
    rank = tables[0].shape[2]
    counts = [t.shape[0] for t in tables]
    out = jax.ShapeDtypeStruct((users // CORES, rank + 8, rank), F32)
    whole = pl.BlockSpec(memory_space=pltpu.VMEM)
    operands = [code, *tables, *before]
    pairs = users * sum(counts)
    return pl.pallas_call(
        functools.partial(gram_kernel, counts=counts, first=not before, offset=offset),
        grid_spec=pltpu.PrefetchScalarGridSpec(
            num_scalar_prefetch=1,
            grid=(sum(counts),),
            in_specs=[whole for x in operands],
            out_specs=[whole, whole],
            scratch_shapes=[
                pltpu.VMEM((4 * rank, LOW), BF16),
                pltpu.VMEM((users, slots), F32),
                pltpu.VMEM((users, slots), F32),
                pltpu.VMEM((users, slots), F32),
                pltpu.VMEM((users, slots // 2), F32),
                pltpu.VMEM((users, rank + 16, slots), BF16),
            ],
        ),
        out_shape=[out, out],
        cost_estimate=pl.CostEstimate(
            flops=pairs * 2 * slots * (4 * LOW + rank) * rank, transcendentals=0, bytes_accessed=4 * pairs * slots
        ),
        name="gram",
    )(source, *operands)


def solve_kernel(own_ref, other_ref, out_ref, rows_s):
    users, rank = out_ref.shape
    lane = lax.broadcasted_iota(jnp.int32, (users, rank), 1)
    number = jnp.sum(own_ref[:, rank + 1, :] + other_ref[:, rank + 1, :], axis=1, keepdims=True)
    shift = jnp.broadcast_to(0.1 * number / rank, (users, rank))
    for i in range(rank):
        row = own_ref[:, i, :] + other_ref[:, i, :]
        rows_s[i] = jnp.where(lane == i, row + shift, row)
    right = own_ref[:, rank, :] + other_ref[:, rank, :]

    def lane_of(value, i):
        return jnp.broadcast_to(value[:, i : i + 1], (users, rank))

    answer = jnp.zeros((users, rank), F32)
    for start in range(0, rank, PANEL):
        steps = range(PANEL)
        rows = [rows_s[start + t] for t in steps]
        corner = {(t, s): lane_of(rows[s], start + t) for t in steps for s in range(t + 1)}
        middle = [lane_of(right, start + t) for t in steps]
        inside = (lane >= start) & (lane < start + PANEL)
        rows = [jnp.where(inside, jnp.where(lane == start + t, 1.0, 0.0), rows[t]) for t in steps]
        inverse = []
        for s in steps:
            inverse.append(1.0 / corner[s, s])
            for t in range(s + 1, PANEL):
                factor = corner[t, s] * inverse[s]
                for q in range(s + 1, t + 1):
                    corner[t, q] = corner[t, q] - factor * corner[q, s]
                rows[t] = rows[t] - factor * rows[s]
                middle[t] = middle[t] - factor * middle[s]
        for t in steps:
            scaled = middle[t] * inverse[t]
            answer = answer + jnp.where(lane < start + PANEL, scaled * rows[t], 0.0)
            right = right - scaled * rows[t]
        below = [rows[t] * inverse[t] for t in steps]
        for i in range(start + PANEL, rank):
            row = jnp.where(inside, 0.0, rows_s[i])
            for t in steps:
                row = row - lane_of(below[t], i) * rows[t]
            rows_s[i] = row
    out_ref[...] = answer


def solve(own, other):
    users, _, rank = own.shape
    return pl.pallas_call(
        solve_kernel,
        out_shape=jax.ShapeDtypeStruct((users, rank), F32),
        scratch_shapes=[pltpu.VMEM((rank, users, rank), F32)],
        name="solve",
    )(own, other)


def coded(item_index, counts):
    low = item_index % LOW
    value = jnp.where(low < HALF, low + HALF, -low) * (1 << (item_index // LOW))
    position = lax.broadcasted_iota(jnp.int32, item_index.shape, 1)
    return jnp.where(position < counts, value, 0).astype(BF16)


def row_at(y, x, core):
    return (y % SIDE * SIDE + x % SIDE) * CORES + core


def shifted(value, first, by):
    pairs = []
    for y in range(SIDE):
        for x in range(SIDE):
            for core in range(CORES):
                along_x = first == (core == 0)
                to = row_at(y, x + by, core) if along_x else row_at(y + by, x, core)
                pairs.append((row_at(y, x, core), to))
    return lax.ppermute(value, "row", pairs)


def ring(value, first):
    half = value.shape[0] // 2
    behind, ahead = shifted(value, first, 1), shifted(value, first, -1)
    return behind, ahead, shifted(behind[:half], first, 1), shifted(ahead[half:], first, -1)


def half_sweep(item_factors, item_index, ratings, counts):
    n_row, n_col = lax.axis_size("row"), lax.axis_size("col")
    chips = n_row // CORES
    slots = item_index.shape[1]
    me = lax.axis_index("row")
    core = me % CORES

    code = jnp.concatenate([coded(item_index, counts), ratings], axis=1).reshape(chips, CORES, -1, 2 * slots)
    code = jnp.where(core == 0, code, code[:, ::-1]).reshape(chips, -1, 2 * slots)
    same_core = [[chip * CORES + c for chip in range(chips)] for c in range(CORES)]
    code = lax.all_to_all(code, "row", 0, 0, tiled=True, axis_index_groups=same_core)

    copies = jnp.broadcast_to(item_factors.T, (n_col, *item_factors.T.shape))
    block = lax.all_to_all(copies, "col", 0, 0, tiled=True)

    source = jnp.asarray(SOURCES)[me]
    behind, ahead, far_low, far_high = ring(block, True)
    near = jnp.stack([block, behind, ahead, jnp.concatenate([far_low, far_high])])
    own, other = gram(source, 0, code, [near])
    behind, ahead, far_low, far_high = ring(near, False)
    own, other = gram(source, 4, code, [behind, ahead], (own, other))
    own, other = gram(source, 12, code, [far_low, far_high], (own, other))
    other = lax.ppermute(other, "row", [(i, i ^ 1) for i in range(n_row)])
    return solve(own, other)[None]


def sources():
    table = np.zeros((SIDE * SIDE * CORES, SIDE * SIDE), np.int32)
    for y in range(SIDE):
        for x in range(SIDE):
            for core in range(CORES):
                for k, (second, first) in enumerate((b, a) for b in (0, -1, 1, 2) for a in (0, -1, 1, 2)):
                    dx, dy = (first, second) if core == 0 else (second, first)
                    table[row_at(y, x, core), k] = (y + dy) % SIDE * SIDE + (x + dx) % SIDE
    return table


SOURCES = sources()


def solution(mesh):
    return jax.shard_map(
        half_sweep,
        mesh=mesh,
        in_specs=(P(("row", "col"), None), P("col", "row"), P("col", "row"), P("col", "row")),
        out_specs=P("col", "row", None),
        check_vma=False,
    )
```

```python
import functools

import jax
import jax.numpy as jnp
from jax import lax
from jax.experimental import pallas as pl
from jax.experimental.pallas import tpu as pltpu
from jax.sharding import PartitionSpec as P


F32, BF16 = jnp.float32, jnp.bfloat16
LOW = 256
HALF = 128
SIDE = 4
CORES = 2
PANEL = 8
BLOCK = 32
VMEM_BYTES = 16 << 20
ROWS_TO_ROWS = (((1,), (1,)), ((), ()))
COLS_TO_COLS = (((0,), (0,)), ((), ()))


def in_vmem(value):
    return pltpu.with_memory_space_constraint(value, pltpu.VMEM)


def chip_of(me, k):
    core, x, y = me & 1, (me >> 1) & (SIDE - 1), me >> 3

    def away(n):
        return jnp.where(n == 1, -1, jnp.where(n == 2, 1, jnp.where(n == 3, 2, 0)))

    first, second = away(k & 3), away(k >> 2)
    dx, dy = jnp.where(core == 0, first, second), jnp.where(core == 0, second, first)
    return ((y + dy) & (SIDE - 1)) * SIDE + ((x + dx) & (SIDE - 1))


def gram_kernel(me_ref, code_ref, *refs, counts, groups, first, offset):
    tables = refs[: len(counts)]
    before = refs[len(counts) : -6 - len(groups)]
    sums = refs[-6 - len(groups) : -6]
    table_s, low_s, high_s, rate_s, live_s, rows_s = refs[-6:]
    users, slots = low_s.shape
    share = users // len(groups)
    rank = sums[0].shape[2]
    step = pl.program_id(0)

    @pl.when(step == 0)
    def _():
        for n, sum_ref in enumerate(sums):
            sum_ref[...] = jnp.zeros(sum_ref.shape, F32) if first else before[n][...]

    begin = 0
    for table_ref, count in zip(tables, counts):

        @pl.when((step >= begin) & (step < begin + count))
        def _(table_ref=table_ref, begin=begin):
            per = LOW // table_ref.shape[3]
            for z in range(table_ref.shape[1]):
                h, q = z // per, z % per
                table_s[h * rank : (h + 1) * rank, q * 128 : (q + 1) * 128] = table_ref[step - begin, z]

        begin += count

    code = code_ref[chip_of(me_ref[0], offset + step)].astype(F32)
    code = jnp.concatenate([code[n * share : (n + 1) * share] for n in groups], axis=0)
    index = code[:, :slots]
    size = jnp.abs(index)
    above = [jnp.where(size >= LOW * 2**e, 1.0, 0.0) for e in range(3)]
    low_s[...] = index * (1.0 - 0.5 * above[0] - 0.25 * above[1] - 0.125 * above[2])
    high_s[...] = above[0] + above[1] + above[2]
    rate_s[...] = code[:, slots:]
    live = jnp.where(size > 0.0, 1.0, 0.0)
    live_s[...] = live[:, : slots // 2] + live[:, slots // 2 :]

    place = lax.broadcasted_iota(jnp.int32, (LOW, slots), 0)
    row_ids = jnp.where(place < HALF, place + HALF, -place).astype(F32).astype(BF16)
    one, zero = jnp.ones((), BF16), jnp.zeros((), BF16)
    table = table_s[...]
    parts = table.shape[0] // rank
    for u in range(users):
        low = jnp.broadcast_to(low_s[u : u + 1], (16, slots)).astype(BF16)
        low = jnp.concatenate([low] * (LOW // 16), axis=0)
        found = jnp.dot(table, jnp.where(row_ids == low, one, zero), preferred_element_type=F32)
        high = jnp.broadcast_to(high_s[u : u + 1], (rank, slots))
        rows = found[:rank]
        for h in range(1, parts):
            rows = jnp.where(high == h, found[h * rank : (h + 1) * rank], rows)
        rows_s[u, :rank] = rows.astype(BF16)
        rows_s[u, rank:] = jnp.broadcast_to(rate_s[u : u + 1], (16, slots)).astype(BF16)
    tail_row = lax.broadcasted_iota(jnp.int32, (8, rank), 0)
    for u in range(users):
        both = rows_s[u]
        out = lax.dot_general(both, both[:rank], ROWS_TO_ROWS, preferred_element_type=F32)
        sum_ref, v = sums[u // share], u % share
        sum_ref[v, :rank] += out[:rank]
        tail = jnp.where(tail_row == 1, jnp.broadcast_to(live_s[u : u + 1], (8, rank)), out[rank : rank + 8])
        sum_ref[v, rank:] += tail


def gram(me, offset, code, tables, groups, before=()):
    _, users, width = code.shape
    slots, share = width // 2, users // CORES
    rank = tables[0].shape[2]
    counts = [t.shape[0] for t in tables]
    users = share * len(groups)
    out = pltpu.VMEM((share, rank + 8, rank), F32)
    whole = pl.BlockSpec(memory_space=pltpu.VMEM)
    operands = [code, *tables, *before]
    pairs = users * sum(counts)
    return pl.pallas_call(
        functools.partial(gram_kernel, counts=counts, groups=groups, first=not before, offset=offset),
        grid_spec=pltpu.PrefetchScalarGridSpec(
            num_scalar_prefetch=1,
            grid=(sum(counts),),
            in_specs=[whole for x in operands],
            out_specs=[whole for n in groups],
            scratch_shapes=[
                pltpu.VMEM((4 * rank, LOW), BF16),
                pltpu.VMEM((users, slots), F32),
                pltpu.VMEM((users, slots), F32),
                pltpu.VMEM((users, slots), F32),
                pltpu.VMEM((users, slots // 2), F32),
                pltpu.VMEM((users, rank + 16, slots), BF16),
            ],
        ),
        out_shape=[out for n in groups],
        cost_estimate=pl.CostEstimate(
            flops=pairs * 2 * slots * (4 * LOW + rank) * rank, transcendentals=0, bytes_accessed=4 * pairs * slots
        ),
        compiler_params=pltpu.CompilerParams(vmem_limit_bytes=VMEM_BYTES),
        name="gram",
    )(me, *[in_vmem(x) for x in operands])


def solve_kernel(own_ref, other_ref, out_ref, rows_s, below_s):
    users, rank = out_ref.shape
    lane = lax.broadcasted_iota(jnp.int32, (users, rank), 1)
    number = jnp.sum(own_ref[:, rank + 1, :] + other_ref[:, rank + 1, :], axis=1, keepdims=True)
    shift = jnp.broadcast_to(0.1 * number / rank, (users, rank))
    for i in range(rank):
        row = own_ref[:, i, :] + other_ref[:, i, :]
        rows_s[i * users : (i + 1) * users] = jnp.where(lane == i, row + shift, row)
    right = own_ref[:, rank, :] + other_ref[:, rank, :]

    def lane_of(value, i):
        return jnp.broadcast_to(value[:, i : i + 1], (users, rank))

    def row_of(i):
        return slice(i * users, (i + 1) * users)

    answer = jnp.zeros((users, rank), F32)
    steps = range(PANEL)
    for top in range(0, rank, BLOCK):
        end = top + BLOCK
        for start in range(top, end, PANEL):
            rows = [rows_s[row_of(start + t)] for t in steps]
            corner = {(t, s): lane_of(rows[s], start + t) for t in steps for s in range(t + 1)}
            middle = [lane_of(right, start + t) for t in steps]
            inside = (lane >= start) & (lane < start + PANEL)
            rows = [jnp.where(inside, jnp.where(lane == start + t, 1.0, 0.0), rows[t]) for t in steps]
            inverse = []
            for s in steps:
                inverse.append(1.0 / corner[s, s])
                for t in range(s + 1, PANEL):
                    factor = corner[t, s] * inverse[s]
                    for q in range(s + 1, t + 1):
                        corner[t, q] = corner[t, q] - factor * corner[q, s]
                    rows[t] = rows[t] - factor * rows[s]
                    middle[t] = middle[t] - factor * middle[s]
            for t in steps:
                scaled = middle[t] * inverse[t]
                answer = answer + jnp.where(lane < start + PANEL, scaled * rows[t], 0.0)
                right = right - scaled * rows[t]
            below = [rows[t] * inverse[t] for t in steps]
            for i in range(start + PANEL, end):
                row = jnp.where(inside, 0.0, rows_s[row_of(i)])
                for t in steps:
                    row = row - lane_of(below[t], i) * rows[t]
                rows_s[row_of(i)] = row
            if end < rank:
                pending = (lane >= start + PANEL) & (lane < end)
                for t in steps:
                    rows_s[row_of(start + t)] = jnp.where(pending, 0.0, rows[t])
                    below_s[row_of(start + t - top)] = below[t]
        if end < rank:
            wide = lax.broadcasted_iota(jnp.int32, (rank - end, rank), 1)
            within = (wide >= top) & (wide < end)
            for u in range(users):
                factors = below_s[pl.ds(u, BLOCK, stride=users), :]
                upper = rows_s[pl.ds(top * users + u, BLOCK, stride=users), :]
                change = lax.dot_general(
                    factors[:, end:],
                    upper,
                    COLS_TO_COLS,
                    precision=lax.Precision.HIGHEST,
                    preferred_element_type=F32,
                )
                rest = pl.ds(end * users + u, rank - end, stride=users)
                rows_s[rest, :] = jnp.where(within, 0.0, rows_s[rest, :]) - change
    out_ref[...] = answer


def solve(own, other):
    users, _, rank = own.shape
    return pl.pallas_call(
        solve_kernel,
        out_shape=jax.ShapeDtypeStruct((users, rank), F32),
        scratch_shapes=[pltpu.VMEM((rank * users, rank), F32), pltpu.VMEM((BLOCK * users, rank), F32)],
        compiler_params=pltpu.CompilerParams(vmem_limit_bytes=VMEM_BYTES),
        name="solve",
    )(in_vmem(own), in_vmem(other))


def coded(item_index, counts, begin, items):
    item_index = (item_index + (items - begin)) % items
    low = item_index % LOW
    value = jnp.where(low < HALF, low + HALF, -low) * (1 << (item_index // LOW))
    position = lax.broadcasted_iota(jnp.int32, item_index.shape, 1)
    return jnp.where(position < counts, value, 0).astype(BF16)


def row_at(y, x, core):
    return (y % SIDE * SIDE + x % SIDE) * CORES + core


def along_col(value, by):
    size = lax.axis_size("col")
    return lax.ppermute(value, "col", [(i, (i + by) % size) for i in range(size)])


def shifted(value, first, by):
    pairs = []
    for y in range(SIDE):
        for x in range(SIDE):
            for core in range(CORES):
                along_x = first == (core == 0)
                to = row_at(y, x + by, core) if along_x else row_at(y + by, x, core)
                pairs.append((row_at(y, x, core), to))
    return lax.ppermute(value, "row", pairs)


def ring(value, first):
    half = value.shape[0] // 2
    behind, ahead = shifted(value, first, 1), shifted(value, first, -1)
    return behind, ahead, shifted(behind[:half], first, 1), shifted(ahead[half:], first, -1)


def half_sweep(item_factors, item_index, ratings, counts):
    n_row, n_col = lax.axis_size("row"), lax.axis_size("col")
    chips = n_row // CORES
    slots, held = item_index.shape[1], item_factors.shape[0]
    me, z = lax.axis_index("row"), lax.axis_index("col")
    core = me % CORES

    code = coded(item_index, counts, (z + n_col // 2) % n_col * held, n_col * held)
    code = jnp.concatenate([code, ratings], axis=1).reshape(chips, CORES, -1, 2 * slots)
    code = jnp.where(core == 0, code, code[:, ::-1]).reshape(chips, -1, 2 * slots)
    same_core = [[chip * CORES + c for chip in range(chips)] for c in range(CORES)]
    code = lax.all_to_all(code, "row", 0, 0, tiled=True, axis_index_groups=same_core)

    mine = item_factors.T
    three = jnp.stack([along_col(mine, 1), mine, along_col(mine, -1)])
    block = jnp.concatenate([along_col(three, 3), three, along_col(three[:2], -3)])

    who = jnp.full((1,), me, jnp.int32)
    both, own_users, other_users = (0, 1), (0,), (1,)
    behind, ahead, far_low, far_high = ring(block, True)
    near = jnp.stack([block, behind, ahead, jnp.concatenate([far_low, far_high])])
    own, other = gram(who, 0, code, [near], both)
    behind, ahead, far_low, far_high = ring(near, False)
    own, other = gram(who, 4, code, [behind, ahead], both, (own, other))
    (other,) = gram(who, 12, code, [far_low, far_high], other_users, (other,))
    other = lax.ppermute(other, "row", [(i, i ^ 1) for i in range(n_row)])
    (own,) = gram(who, 12, code, [far_low, far_high], own_users, (own,))
    return solve(own, other)[None]


def solution(mesh):
    return jax.shard_map(
        half_sweep,
        mesh=mesh,
        in_specs=(P(("row", "col"), None), P("col", "row"), P("col", "row"), P("col", "row")),
        out_specs=P("col", "row", None),
        check_vma=False,
    )
```

```python
import functools

import jax
import jax.numpy as jnp
from jax import lax
from jax.experimental import pallas as pl
from jax.experimental.pallas import tpu as pltpu
from jax.sharding import PartitionSpec as P


F32, BF16 = jnp.float32, jnp.bfloat16
LOW = 256
HALF = 128
SIDE = 4
CORES = 2
PANEL = 8
BLOCK = 32
VMEM_BYTES = 16 << 20
ROWS_TO_ROWS = (((1,), (1,)), ((), ()))
COLS_TO_COLS = (((0,), (0,)), ((), ()))


def in_vmem(value):
    return pltpu.with_memory_space_constraint(value, pltpu.VMEM)


def chip_of(me, k):
    core, x, y = me & 1, (me >> 1) & (SIDE - 1), me >> 3

    def away(n):
        return jnp.where(n == 1, -1, jnp.where(n == 2, 1, jnp.where(n == 3, 2, 0)))

    first, second = away(k & 3), away(k >> 2)
    dx, dy = jnp.where(core == 0, first, second), jnp.where(core == 0, second, first)
    return ((y + dy) & (SIDE - 1)) * SIDE + ((x + dx) & (SIDE - 1))


def gram_kernel(me_ref, code_ref, *refs, counts, groups, first, offset):
    tables = refs[: len(counts)]
    before = refs[len(counts) : -6 - len(groups)]
    sums = refs[-6 - len(groups) : -6]
    table_s, low_s, high_s, rate_s, live_s, rows_s = refs[-6:]
    users, slots = low_s.shape
    share = users // len(groups)
    rank = sums[0].shape[2]
    step = pl.program_id(0)

    @pl.when(step == 0)
    def _():
        for n, sum_ref in enumerate(sums):
            sum_ref[...] = jnp.zeros(sum_ref.shape, F32) if first else before[n][...]

    begin = 0
    for table_ref, count in zip(tables, counts):

        @pl.when((step >= begin) & (step < begin + count))
        def _(table_ref=table_ref, begin=begin):
            per = LOW // table_ref.shape[3]
            for z in range(table_ref.shape[1]):
                h, q = z // per, z % per
                table_s[h * rank : (h + 1) * rank, q * 128 : (q + 1) * 128] = table_ref[step - begin, z]

        begin += count

    code = code_ref[chip_of(me_ref[0], offset + step)].astype(F32)
    code = jnp.concatenate([code[n * share : (n + 1) * share] for n in groups], axis=0)
    index = code[:, :slots]
    size = jnp.abs(index)
    above = [jnp.where(size >= LOW * 2**e, 1.0, 0.0) for e in range(3)]
    low_s[...] = index * (1.0 - 0.5 * above[0] - 0.25 * above[1] - 0.125 * above[2])
    high_s[...] = above[0] + above[1] + above[2]
    rate_s[...] = code[:, slots:]
    live = jnp.where(size > 0.0, 1.0, 0.0)
    live_s[...] = live[:, : slots // 2] + live[:, slots // 2 :]

    place = lax.broadcasted_iota(jnp.int32, (LOW, slots), 0)
    row_ids = jnp.where(place < HALF, place + HALF, -place).astype(F32).astype(BF16)
    one, zero = jnp.ones((), BF16), jnp.zeros((), BF16)
    table = table_s[...]
    parts = table.shape[0] // rank
    for u in range(users):
        low = jnp.broadcast_to(low_s[u : u + 1], (16, slots)).astype(BF16)
        low = jnp.concatenate([low] * (LOW // 16), axis=0)
        found = jnp.dot(table, jnp.where(row_ids == low, one, zero), preferred_element_type=F32)
        high = jnp.broadcast_to(high_s[u : u + 1], (rank, slots))
        rows = found[:rank]
        for h in range(1, parts):
            rows = jnp.where(high == h, found[h * rank : (h + 1) * rank], rows)
        rows_s[u, :rank] = rows.astype(BF16)
        rows_s[u, rank:] = jnp.broadcast_to(rate_s[u : u + 1], (16, slots)).astype(BF16)
    tail_row = lax.broadcasted_iota(jnp.int32, (8, rank), 0)
    for u in range(users):
        both = rows_s[u]
        out = lax.dot_general(both, both[:rank], ROWS_TO_ROWS, preferred_element_type=F32)
        sum_ref, v = sums[u // share], u % share
        sum_ref[v, :rank] += out[:rank]
        tail = jnp.where(tail_row == 1, jnp.broadcast_to(live_s[u : u + 1], (8, rank)), out[rank : rank + 8])
        sum_ref[v, rank:] += tail


def gram(me, offset, code, tables, groups, before=()):
    _, users, width = code.shape
    slots, share = width // 2, users // CORES
    rank = tables[0].shape[2]
    counts = [t.shape[0] for t in tables]
    users = share * len(groups)
    out = pltpu.VMEM((share, rank + 8, rank), F32)
    whole = pl.BlockSpec(memory_space=pltpu.VMEM)
    operands = [code, *tables, *before]
    pairs = users * sum(counts)
    return pl.pallas_call(
        functools.partial(gram_kernel, counts=counts, groups=groups, first=not before, offset=offset),
        grid_spec=pltpu.PrefetchScalarGridSpec(
            num_scalar_prefetch=1,
            grid=(sum(counts),),
            in_specs=[whole for x in operands],
            out_specs=[whole for n in groups],
            scratch_shapes=[
                pltpu.VMEM((4 * rank, LOW), BF16),
                pltpu.VMEM((users, slots), F32),
                pltpu.VMEM((users, slots), F32),
                pltpu.VMEM((users, slots), F32),
                pltpu.VMEM((users, slots // 2), F32),
                pltpu.VMEM((users, rank + 16, slots), BF16),
            ],
        ),
        out_shape=[out for n in groups],
        cost_estimate=pl.CostEstimate(
            flops=pairs * 2 * slots * (4 * LOW + rank) * rank, transcendentals=0, bytes_accessed=4 * pairs * slots
        ),
        compiler_params=pltpu.CompilerParams(vmem_limit_bytes=VMEM_BYTES),
        name="gram",
    )(me, *[in_vmem(x) for x in operands])


def solve_kernel(own_ref, other_ref, out_ref, rows_s, below_s):
    users, rank = out_ref.shape
    lane = lax.broadcasted_iota(jnp.int32, (users, rank), 1)
    number = jnp.sum(own_ref[:, rank + 1, :] + other_ref[:, rank + 1, :], axis=1, keepdims=True)
    shift = jnp.broadcast_to(0.1 * number / rank, (users, rank))
    for i in range(rank):
        row = own_ref[:, i, :] + other_ref[:, i, :]
        rows_s[i * users : (i + 1) * users] = jnp.where(lane == i, row + shift, row)
    right = own_ref[:, rank, :] + other_ref[:, rank, :]

    def lane_of(value, i):
        return jnp.broadcast_to(value[:, i : i + 1], (users, rank))

    def row_of(i):
        return slice(i * users, (i + 1) * users)

    answer = jnp.zeros((users, rank), F32)
    steps = range(PANEL)
    for top in range(0, rank, BLOCK):
        end = top + BLOCK
        for start in range(top, end, PANEL):
            rows = [rows_s[row_of(start + t)] for t in steps]
            corner = {(t, s): lane_of(rows[s], start + t) for t in steps for s in range(t + 1)}
            middle = [lane_of(right, start + t) for t in steps]
            inside = (lane >= start) & (lane < start + PANEL)
            rows = [jnp.where(inside, jnp.where(lane == start + t, 1.0, 0.0), rows[t]) for t in steps]
            inverse = []
            for s in steps:
                inverse.append(1.0 / corner[s, s])
                for t in range(s + 1, PANEL):
                    factor = corner[t, s] * inverse[s]
                    for q in range(s + 1, t + 1):
                        corner[t, q] = corner[t, q] - factor * corner[q, s]
                    rows[t] = rows[t] - factor * rows[s]
                    middle[t] = middle[t] - factor * middle[s]
            for t in steps:
                scaled = middle[t] * inverse[t]
                answer = answer + jnp.where(lane < start + PANEL, scaled * rows[t], 0.0)
                right = right - scaled * rows[t]
            below = [rows[t] * inverse[t] for t in steps]
            for i in range(start + PANEL, end):
                row = jnp.where(inside, 0.0, rows_s[row_of(i)])
                for t in steps:
                    row = row - lane_of(below[t], i) * rows[t]
                rows_s[row_of(i)] = row
            if end < rank:
                pending = (lane >= start + PANEL) & (lane < end)
                for t in steps:
                    rows_s[row_of(start + t)] = jnp.where(pending, 0.0, rows[t])
                    below_s[row_of(start + t - top)] = below[t]
        if end < rank:
            wide = lax.broadcasted_iota(jnp.int32, (rank - end, rank), 1)
            within = (wide >= top) & (wide < end)
            for u in range(users):
                factors = below_s[pl.ds(u, BLOCK, stride=users), :]
                upper = rows_s[pl.ds(top * users + u, BLOCK, stride=users), :]
                change = lax.dot_general(
                    factors[:, end:],
                    upper,
                    COLS_TO_COLS,
                    precision=lax.Precision.HIGHEST,
                    preferred_element_type=F32,
                )
                rest = pl.ds(end * users + u, rank - end, stride=users)
                rows_s[rest, :] = jnp.where(within, 0.0, rows_s[rest, :]) - change
    out_ref[...] = answer


def solve(own, other):
    users, _, rank = own.shape
    return pl.pallas_call(
        solve_kernel,
        out_shape=jax.ShapeDtypeStruct((users, rank), F32),
        scratch_shapes=[pltpu.VMEM((rank * users, rank), F32), pltpu.VMEM((BLOCK * users, rank), F32)],
        compiler_params=pltpu.CompilerParams(vmem_limit_bytes=VMEM_BYTES),
        name="solve",
    )(in_vmem(own), in_vmem(other))


def coded(item_index, counts, begin, items):
    item_index = (item_index + (items - begin)) % items
    low = item_index % LOW
    value = jnp.where(low < HALF, low + HALF, -low) * (1 << (item_index // LOW))
    position = lax.broadcasted_iota(jnp.int32, item_index.shape, 1)
    return jnp.where(position < counts, value, 0).astype(BF16)


def row_at(y, x, core):
    return (y % SIDE * SIDE + x % SIDE) * CORES + core


def along_col(value, by):
    size = lax.axis_size("col")
    return lax.ppermute(value, "col", [(i, (i + by) % size) for i in range(size)])


def shifted(value, first, by):
    pairs = []
    for y in range(SIDE):
        for x in range(SIDE):
            for core in range(CORES):
                along_x = first == (core == 0)
                to = row_at(y, x + by, core) if along_x else row_at(y + by, x, core)
                pairs.append((row_at(y, x, core), to))
    return lax.ppermute(value, "row", pairs)


def near_of(value, first):
    return shifted(value, first, 1), shifted(value, first, -1)


def far_of(low, high, first):
    return shifted(low, first, 1), shifted(high, first, -1)


def half_sweep(item_factors, item_index, ratings, counts):
    n_row, n_col = lax.axis_size("row"), lax.axis_size("col")
    chips = n_row // CORES
    slots, held = item_index.shape[1], item_factors.shape[0]
    me, z = lax.axis_index("row"), lax.axis_index("col")
    core = me % CORES

    code = coded(item_index, counts, (z + n_col // 2) % n_col * held, n_col * held)
    code = jnp.concatenate([code, ratings], axis=1).reshape(chips, CORES, -1, 2 * slots)
    code = jnp.where(core == 0, code, code[:, ::-1]).reshape(chips, -1, 2 * slots)
    same_core = [[chip * CORES + c for chip in range(chips)] for c in range(CORES)]
    code = lax.all_to_all(code, "row", 0, 0, tiled=True, axis_index_groups=same_core)

    mine = item_factors.T
    three = jnp.stack([along_col(mine, 1), mine, along_col(mine, -1)])
    block = jnp.concatenate([along_col(three, 3), three, along_col(three[:2], -3)])

    who = jnp.full((1,), me, jnp.int32)
    both, own_users, other_users = (0, 1), (0,), (1,)
    half = n_col // 2
    behind, ahead = near_of(block, True)
    alone = block[None]
    alone_behind, alone_ahead = near_of(alone, False)
    far = jnp.concatenate(far_of(behind[:half], ahead[half:], True))[None]
    sides = jnp.stack([behind, ahead])
    sides_behind, sides_ahead = near_of(sides, False)
    far_behind, far_ahead = near_of(far, False)
    own, other = gram(who, 0, code, [alone, sides, far], both)
    low, high = far_of(
        jnp.concatenate([alone_behind, sides_behind[:1]]), jnp.concatenate([sides_ahead[1:], far_ahead]), False
    )
    tables = [alone_behind, sides_behind, far_behind, alone_ahead, sides_ahead, far_ahead]
    own, other = gram(who, 4, code, tables, both, (own, other))
    (other,) = gram(who, 12, code, [low, high], other_users, (other,))
    other = lax.ppermute(other, "row", [(i, i ^ 1) for i in range(n_row)])
    (own,) = gram(who, 12, code, [low, high], own_users, (own,))
    return solve(own, other)[None]


def solution(mesh):
    return jax.shard_map(
        half_sweep,
        mesh=mesh,
        in_specs=(P(("row", "col"), None), P("col", "row"), P("col", "row"), P("col", "row")),
        out_specs=P("col", "row", None),
        check_vma=False,
    )
```

```python
import functools

import jax
import jax.numpy as jnp
from jax import lax
from jax.experimental import pallas as pl
from jax.experimental.pallas import tpu as pltpu
from jax.sharding import PartitionSpec as P


F32, BF16 = jnp.float32, jnp.bfloat16
LOW = 256
HALF = 128
SIDE = 4
CORES = 2
PANEL = 8
BLOCK = 32
VMEM_BYTES = 16 << 20
ROWS_TO_ROWS = (((1,), (1,)), ((), ()))
COLS_TO_COLS = (((0,), (0,)), ((), ()))


def in_vmem(value):
    return pltpu.with_memory_space_constraint(value, pltpu.VMEM)


def chip_of(me, k):
    core, x, y = me & 1, (me >> 1) & (SIDE - 1), me >> 3

    def away(n):
        return jnp.where(n == 1, -1, jnp.where(n == 2, 1, jnp.where(n == 3, 2, 0)))

    first, second = away(k & 3), away(k >> 2)
    dx, dy = jnp.where(core == 0, first, second), jnp.where(core == 0, second, first)
    return ((y + dy) & (SIDE - 1)) * SIDE + ((x + dx) & (SIDE - 1))


def gram_kernel(me_ref, code_ref, *refs, counts, groups, first, offset):
    tables = refs[: len(counts)]
    before = refs[len(counts) : -6 - len(groups)]
    sums = refs[-6 - len(groups) : -6]
    table_s, low_s, high_s, rate_s, live_s, rows_s = refs[-6:]
    users, slots = low_s.shape
    share = users // len(groups)
    rank = sums[0].shape[2]
    step = pl.program_id(0)

    @pl.when(step == 0)
    def _():
        for n, sum_ref in enumerate(sums):
            sum_ref[...] = jnp.zeros(sum_ref.shape, F32) if first else before[n][...]

    begin = 0
    for table_ref, count in zip(tables, counts):

        @pl.when((step >= begin) & (step < begin + count))
        def _(table_ref=table_ref, begin=begin):
            per = LOW // table_ref.shape[3]
            for z in range(table_ref.shape[1]):
                h, q = z // per, z % per
                table_s[h * rank : (h + 1) * rank, q * 128 : (q + 1) * 128] = table_ref[step - begin, z]

        begin += count

    code = code_ref[chip_of(me_ref[0], offset + step)].astype(F32)
    code = jnp.concatenate([code[n * share : (n + 1) * share] for n in groups], axis=0)
    index = code[:, :slots]
    size = jnp.abs(index)
    above = [jnp.where(size >= LOW * 2**e, 1.0, 0.0) for e in range(3)]
    low_s[...] = index * (1.0 - 0.5 * above[0] - 0.25 * above[1] - 0.125 * above[2])
    high_s[...] = above[0] + above[1] + above[2]
    rate_s[...] = code[:, slots:]
    live = jnp.where(size > 0.0, 1.0, 0.0)
    live_s[...] = live[:, : slots // 2] + live[:, slots // 2 :]

    place = lax.broadcasted_iota(jnp.int32, (LOW, slots), 0)
    row_ids = jnp.where(place < HALF, place + HALF, -place).astype(F32).astype(BF16)
    one, zero = jnp.ones((), BF16), jnp.zeros((), BF16)
    table = table_s[...]
    parts = table.shape[0] // rank
    for u in range(users):
        low = jnp.broadcast_to(low_s[u : u + 1], (16, slots)).astype(BF16)
        low = jnp.concatenate([low] * (LOW // 16), axis=0)
        found = jnp.dot(table, jnp.where(row_ids == low, one, zero), preferred_element_type=F32)
        high = jnp.broadcast_to(high_s[u : u + 1], (rank, slots))
        rows = found[:rank]
        for h in range(1, parts):
            rows = jnp.where(high == h, found[h * rank : (h + 1) * rank], rows)
        rows_s[u, :rank] = rows.astype(BF16)
        rows_s[u, rank:] = jnp.broadcast_to(rate_s[u : u + 1], (16, slots)).astype(BF16)
    tail_row = lax.broadcasted_iota(jnp.int32, (8, rank), 0)
    for u in range(users):
        both = rows_s[u]
        out = lax.dot_general(both, both[:rank], ROWS_TO_ROWS, preferred_element_type=F32)
        sum_ref, v = sums[u // share], u % share
        sum_ref[v, :rank] += out[:rank]
        tail = jnp.where(tail_row == 1, jnp.broadcast_to(live_s[u : u + 1], (8, rank)), out[rank : rank + 8])
        sum_ref[v, rank:] += tail


def gram(me, offset, code, tables, groups, before=()):
    _, users, width = code.shape
    slots, share = width // 2, users // CORES
    rank = tables[0].shape[2]
    counts = [t.shape[0] for t in tables]
    users = share * len(groups)
    out = pltpu.VMEM((share, rank + 8, rank), F32)
    whole = pl.BlockSpec(memory_space=pltpu.VMEM)
    operands = [code, *tables, *before]
    pairs = users * sum(counts)
    return pl.pallas_call(
        functools.partial(gram_kernel, counts=counts, groups=groups, first=not before, offset=offset),
        grid_spec=pltpu.PrefetchScalarGridSpec(
            num_scalar_prefetch=1,
            grid=(sum(counts),),
            in_specs=[whole for x in operands],
            out_specs=[whole for n in groups],
            scratch_shapes=[
                pltpu.VMEM((4 * rank, LOW), BF16),
                pltpu.VMEM((users, slots), F32),
                pltpu.VMEM((users, slots), F32),
                pltpu.VMEM((users, slots), F32),
                pltpu.VMEM((users, slots // 2), F32),
                pltpu.VMEM((users, rank + 16, slots), BF16),
            ],
        ),
        out_shape=[out for n in groups],
        cost_estimate=pl.CostEstimate(
            flops=pairs * 2 * slots * (4 * LOW + rank) * rank, transcendentals=0, bytes_accessed=4 * pairs * slots
        ),
        compiler_params=pltpu.CompilerParams(vmem_limit_bytes=VMEM_BYTES),
        name="gram",
    )(me, *[in_vmem(x) for x in operands])


def solve_kernel(own_ref, other_ref, out_ref, rows_s, below_s):
    users, rank = out_ref.shape
    lane = lax.broadcasted_iota(jnp.int32, (users, rank), 1)
    number = jnp.sum(own_ref[:, rank + 1, :] + other_ref[:, rank + 1, :], axis=1, keepdims=True)
    shift = jnp.broadcast_to(0.1 * number / rank, (users, rank))
    for i in range(rank):
        row = own_ref[:, i, :] + other_ref[:, i, :]
        rows_s[i * users : (i + 1) * users] = jnp.where(lane == i, row + shift, row)
    right = own_ref[:, rank, :] + other_ref[:, rank, :]

    def lane_of(value, i):
        return jnp.broadcast_to(value[:, i : i + 1], (users, rank))

    def row_of(i):
        return slice(i * users, (i + 1) * users)

    answer = jnp.zeros((users, rank), F32)
    steps = range(PANEL)
    for top in range(0, rank, BLOCK):
        end = top + BLOCK
        for start in range(top, end, PANEL):
            rows = [rows_s[row_of(start + t)] for t in steps]
            corner = {(t, s): lane_of(rows[s], start + t) for t in steps for s in range(t + 1)}
            middle = [lane_of(right, start + t) for t in steps]
            inside = (lane >= start) & (lane < start + PANEL)
            rows = [jnp.where(inside, jnp.where(lane == start + t, 1.0, 0.0), rows[t]) for t in steps]
            inverse = []
            for s in steps:
                inverse.append(1.0 / corner[s, s])
                for t in range(s + 1, PANEL):
                    factor = corner[t, s] * inverse[s]
                    for q in range(s + 1, t + 1):
                        corner[t, q] = corner[t, q] - factor * corner[q, s]
                    rows[t] = rows[t] - factor * rows[s]
                    middle[t] = middle[t] - factor * middle[s]
            for t in steps:
                scaled = middle[t] * inverse[t]
                answer = answer + jnp.where(lane < start + PANEL, scaled * rows[t], 0.0)
                right = right - scaled * rows[t]
            below = [rows[t] * inverse[t] for t in steps]
            for i in range(start + PANEL, end):
                row = jnp.where(inside, 0.0, rows_s[row_of(i)])
                for t in steps:
                    row = row - lane_of(below[t], i) * rows[t]
                rows_s[row_of(i)] = row
            if end < rank:
                pending = (lane >= start + PANEL) & (lane < end)
                for t in steps:
                    rows_s[row_of(start + t)] = jnp.where(pending, 0.0, rows[t])
                    below_s[row_of(start + t - top)] = below[t]
        if end < rank:
            wide = lax.broadcasted_iota(jnp.int32, (rank - end, rank), 1)
            within = (wide >= top) & (wide < end)
            for u in range(users):
                factors = below_s[pl.ds(u, BLOCK, stride=users), :]
                upper = rows_s[pl.ds(top * users + u, BLOCK, stride=users), :]
                change = lax.dot_general(
                    factors[:, end:],
                    upper,
                    COLS_TO_COLS,
                    precision=lax.Precision.HIGHEST,
                    preferred_element_type=F32,
                )
                rest = pl.ds(end * users + u, rank - end, stride=users)
                rows_s[rest, :] = jnp.where(within, 0.0, rows_s[rest, :]) - change
    out_ref[...] = answer


def solve(own, other):
    users, _, rank = own.shape
    return pl.pallas_call(
        solve_kernel,
        out_shape=jax.ShapeDtypeStruct((users, rank), F32),
        scratch_shapes=[pltpu.VMEM((rank * users, rank), F32), pltpu.VMEM((BLOCK * users, rank), F32)],
        compiler_params=pltpu.CompilerParams(vmem_limit_bytes=VMEM_BYTES),
        name="solve",
    )(in_vmem(own), in_vmem(other))


def coded(item_index, counts, begin, items):
    item_index = (item_index + (items - begin)) % items
    low = item_index % LOW
    value = jnp.where(low < HALF, low + HALF, -low) * (1 << (item_index // LOW))
    position = lax.broadcasted_iota(jnp.int32, item_index.shape, 1)
    return jnp.where(position < counts, value, 0).astype(BF16)


def row_at(y, x, core):
    return (y % SIDE * SIDE + x % SIDE) * CORES + core


def along_col(value, by):
    size = lax.axis_size("col")
    return lax.ppermute(value, "col", [(i, (i + by) % size) for i in range(size)])


def shifted(value, first, by):
    pairs = []
    for y in range(SIDE):
        for x in range(SIDE):
            for core in range(CORES):
                along_x = first == (core == 0)
                to = row_at(y, x + by, core) if along_x else row_at(y + by, x, core)
                pairs.append((row_at(y, x, core), to))
    return lax.ppermute(value, "row", pairs)


def near_of(value, first):
    return shifted(value, first, 1), shifted(value, first, -1)


def far_of(low, high, first):
    return shifted(low, first, 1), shifted(high, first, -1)


def half_sweep(item_factors, item_index, ratings, counts):
    n_row, n_col = lax.axis_size("row"), lax.axis_size("col")
    chips = n_row // CORES
    slots, held = item_index.shape[1], item_factors.shape[0]
    me, z = lax.axis_index("row"), lax.axis_index("col")
    core = me % CORES

    code = coded(item_index, counts, (z + n_col // 2) % n_col * held, n_col * held)
    code = jnp.concatenate([code, ratings], axis=1).reshape(chips, CORES, -1, 2 * slots)
    code = jnp.where(core == 0, code, code[:, ::-1]).reshape(chips, -1, 2 * slots)
    same_core = [[chip * CORES + c for chip in range(chips)] for c in range(CORES)]
    code = lax.all_to_all(code, "row", 0, 0, tiled=True, axis_index_groups=same_core)

    mine = item_factors.T
    three = jnp.stack([along_col(mine, 1), mine, along_col(mine, -1)])
    block = jnp.concatenate([along_col(three, 3), three, along_col(three[:2], -3)])

    who = jnp.full((1,), me, jnp.int32)
    both, own_users, other_users = (0, 1), (0,), (1,)
    half = n_col // 2
    behind, ahead = near_of(block, True)
    three = jnp.stack([block, behind, ahead])
    three_behind, three_ahead = near_of(three, False)
    far = jnp.concatenate(far_of(behind[:half], ahead[half:], True))[None]
    own, other = gram(who, 0, code, [three], both)
    far_behind, far_ahead = near_of(far, False)
    own, other = gram(who, 3, code, [far], both, (own, other))
    low, high = far_of(three_behind[:2], jnp.concatenate([three_ahead[2:], far_ahead]), False)
    tables = [three_behind, far_behind, three_ahead, far_ahead]
    own, other = gram(who, 4, code, tables, both, (own, other))
    (other,) = gram(who, 12, code, [low, high], other_users, (other,))
    other = lax.ppermute(other, "row", [(i, i ^ 1) for i in range(n_row)])
    (own,) = gram(who, 12, code, [low, high], own_users, (own,))
    return solve(own, other)[None]


def solution(mesh):
    return jax.shard_map(
        half_sweep,
        mesh=mesh,
        in_specs=(P(("row", "col"), None), P("col", "row"), P("col", "row"), P("col", "row")),
        out_specs=P("col", "row", None),
        check_vma=False,
    )
```

```python
import functools

import jax
import jax.numpy as jnp
from jax import lax
from jax.experimental import pallas as pl
from jax.experimental.pallas import tpu as pltpu
from jax.sharding import PartitionSpec as P


F32, BF16 = jnp.float32, jnp.bfloat16
LOW = 256
HALF = 128
SIDE = 4
CORES = 2
PANEL = 8
BLOCK = 32
VMEM_BYTES = 16 << 20
ROWS_TO_ROWS = (((1,), (1,)), ((), ()))
COLS_TO_COLS = (((0,), (0,)), ((), ()))


def in_vmem(value):
    return pltpu.with_memory_space_constraint(value, pltpu.VMEM)


def chip_of(me, k):
    core, x, y = me & 1, (me >> 1) & (SIDE - 1), me >> 3

    def away(n):
        return jnp.where(n == 1, -1, jnp.where(n == 2, 1, jnp.where(n == 3, 2, 0)))

    first, second = away(k & 3), away(k >> 2)
    dx, dy = jnp.where(core == 0, first, second), jnp.where(core == 0, second, first)
    return ((y + dy) & (SIDE - 1)) * SIDE + ((x + dx) & (SIDE - 1))


def gram_kernel(me_ref, code_ref, *refs, counts, groups, first, offset):
    tables = refs[: len(counts)]
    before = refs[len(counts) : -6 - len(groups)]
    sums = refs[-6 - len(groups) : -6]
    table_s, low_s, high_s, rate_s, live_s, rows_s = refs[-6:]
    users, slots = low_s.shape
    share = users // len(groups)
    rank = sums[0].shape[2]
    step = pl.program_id(0)

    @pl.when(step == 0)
    def _():
        for n, sum_ref in enumerate(sums):
            sum_ref[...] = jnp.zeros(sum_ref.shape, F32) if first else before[n][...]

    begin = 0
    for table_ref, count in zip(tables, counts):

        @pl.when((step >= begin) & (step < begin + count))
        def _(table_ref=table_ref, begin=begin):
            per = LOW // table_ref.shape[3]
            for z in range(table_ref.shape[1]):
                h, q = z // per, z % per
                table_s[h * rank : (h + 1) * rank, q * 128 : (q + 1) * 128] = table_ref[step - begin, z]

        begin += count

    code = code_ref[chip_of(me_ref[0], offset + step)].astype(F32)
    code = jnp.concatenate([code[n * share : (n + 1) * share] for n in groups], axis=0)
    index = code[:, :slots]
    size = jnp.abs(index)
    above = [jnp.where(size >= LOW * 2**e, 1.0, 0.0) for e in range(3)]
    low_s[...] = index * (1.0 - 0.5 * above[0] - 0.25 * above[1] - 0.125 * above[2])
    high_s[...] = above[0] + above[1] + above[2]
    rate_s[...] = code[:, slots:]
    live = jnp.where(size > 0.0, 1.0, 0.0)
    live_s[...] = live[:, : slots // 2] + live[:, slots // 2 :]

    place = lax.broadcasted_iota(jnp.int32, (LOW, slots), 0)
    row_ids = jnp.where(place < HALF, place + HALF, -place).astype(F32).astype(BF16)
    one, zero = jnp.ones((), BF16), jnp.zeros((), BF16)
    table = table_s[...]
    parts = table.shape[0] // rank
    for u in range(users):
        low = jnp.broadcast_to(low_s[u : u + 1], (16, slots)).astype(BF16)
        low = jnp.concatenate([low] * (LOW // 16), axis=0)
        found = jnp.dot(table, jnp.where(row_ids == low, one, zero), preferred_element_type=F32)
        high = jnp.broadcast_to(high_s[u : u + 1], (rank, slots))
        rows = found[:rank]
        for h in range(1, parts):
            rows = jnp.where(high == h, found[h * rank : (h + 1) * rank], rows)
        rows_s[u, :rank] = rows.astype(BF16)
        rows_s[u, rank:] = jnp.broadcast_to(rate_s[u : u + 1], (16, slots)).astype(BF16)
    tail_row = lax.broadcasted_iota(jnp.int32, (8, rank), 0)
    for u in range(users):
        both = rows_s[u]
        out = lax.dot_general(both, both[:rank], ROWS_TO_ROWS, preferred_element_type=F32)
        sum_ref, v = sums[u // share], u % share
        sum_ref[v, :rank] += out[:rank]
        tail = jnp.where(tail_row == 1, jnp.broadcast_to(live_s[u : u + 1], (8, rank)), out[rank : rank + 8])
        sum_ref[v, rank:] += tail


def gram(me, offset, code, tables, groups, before=()):
    _, users, width = code.shape
    slots, share = width // 2, users // CORES
    rank = tables[0].shape[2]
    counts = [t.shape[0] for t in tables]
    users = share * len(groups)
    out = pltpu.VMEM((share, rank + 8, rank), F32)
    whole = pl.BlockSpec(memory_space=pltpu.VMEM)
    operands = [code, *tables, *before]
    pairs = users * sum(counts)
    return pl.pallas_call(
        functools.partial(gram_kernel, counts=counts, groups=groups, first=not before, offset=offset),
        grid_spec=pltpu.PrefetchScalarGridSpec(
            num_scalar_prefetch=1,
            grid=(sum(counts),),
            in_specs=[whole for x in operands],
            out_specs=[whole for n in groups],
            scratch_shapes=[
                pltpu.VMEM((4 * rank, LOW), BF16),
                pltpu.VMEM((users, slots), F32),
                pltpu.VMEM((users, slots), F32),
                pltpu.VMEM((users, slots), F32),
                pltpu.VMEM((users, slots // 2), F32),
                pltpu.VMEM((users, rank + 16, slots), BF16),
            ],
        ),
        out_shape=[out for n in groups],
        cost_estimate=pl.CostEstimate(
            flops=pairs * 2 * slots * (4 * LOW + rank) * rank, transcendentals=0, bytes_accessed=4 * pairs * slots
        ),
        compiler_params=pltpu.CompilerParams(vmem_limit_bytes=VMEM_BYTES),
        name="gram",
    )(me, *[in_vmem(x) for x in operands])


def solve_kernel(own_ref, other_ref, out_ref, rows_s, below_s):
    users, rank = out_ref.shape
    lane = lax.broadcasted_iota(jnp.int32, (users, rank), 1)
    number = jnp.sum(own_ref[:, rank + 1, :] + other_ref[:, rank + 1, :], axis=1, keepdims=True)
    shift = jnp.broadcast_to(0.1 * number / rank, (users, rank))
    for i in range(rank):
        row = own_ref[:, i, :] + other_ref[:, i, :]
        rows_s[i * users : (i + 1) * users] = jnp.where(lane == i, row + shift, row)
    right = own_ref[:, rank, :] + other_ref[:, rank, :]

    def lane_of(value, i):
        return jnp.broadcast_to(value[:, i : i + 1], (users, rank))

    def row_of(i):
        return slice(i * users, (i + 1) * users)

    answer = jnp.zeros((users, rank), F32)
    steps = range(PANEL)
    for top in range(0, rank, BLOCK):
        end = top + BLOCK
        for start in range(top, end, PANEL):
            rows = [rows_s[row_of(start + t)] for t in steps]
            corner = {(t, s): lane_of(rows[s], start + t) for t in steps for s in range(t + 1)}
            middle = [lane_of(right, start + t) for t in steps]
            inside = (lane >= start) & (lane < start + PANEL)
            rows = [jnp.where(inside, jnp.where(lane == start + t, 1.0, 0.0), rows[t]) for t in steps]
            inverse = []
            for s in steps:
                inverse.append(1.0 / corner[s, s])
                for t in range(s + 1, PANEL):
                    factor = corner[t, s] * inverse[s]
                    for q in range(s + 1, t + 1):
                        corner[t, q] = corner[t, q] - factor * corner[q, s]
                    rows[t] = rows[t] - factor * rows[s]
                    middle[t] = middle[t] - factor * middle[s]
            for t in steps:
                scaled = middle[t] * inverse[t]
                answer = answer + jnp.where(lane < start + PANEL, scaled * rows[t], 0.0)
                right = right - scaled * rows[t]
            below = [rows[t] * inverse[t] for t in steps]
            for i in range(start + PANEL, end):
                row = jnp.where(inside, 0.0, rows_s[row_of(i)])
                for t in steps:
                    row = row - lane_of(below[t], i) * rows[t]
                rows_s[row_of(i)] = row
            if end < rank:
                pending = (lane >= start + PANEL) & (lane < end)
                for t in steps:
                    rows_s[row_of(start + t)] = jnp.where(pending, 0.0, rows[t])
                    below_s[row_of(start + t - top)] = below[t]
        if end < rank:
            wide = lax.broadcasted_iota(jnp.int32, (rank - end, rank), 1)
            within = (wide >= top) & (wide < end)
            for u in range(users):
                factors = below_s[pl.ds(u, BLOCK, stride=users), :]
                upper = rows_s[pl.ds(top * users + u, BLOCK, stride=users), :]
                change = lax.dot_general(
                    factors[:, end:],
                    upper,
                    COLS_TO_COLS,
                    precision=lax.Precision.HIGHEST,
                    preferred_element_type=F32,
                )
                rest = pl.ds(end * users + u, rank - end, stride=users)
                rows_s[rest, :] = jnp.where(within, 0.0, rows_s[rest, :]) - change
    out_ref[...] = answer


def solve(own, other):
    users, _, rank = own.shape
    return pl.pallas_call(
        solve_kernel,
        out_shape=jax.ShapeDtypeStruct((users, rank), F32),
        scratch_shapes=[pltpu.VMEM((rank * users, rank), F32), pltpu.VMEM((BLOCK * users, rank), F32)],
        compiler_params=pltpu.CompilerParams(vmem_limit_bytes=VMEM_BYTES),
        name="solve",
    )(in_vmem(own), in_vmem(other))


def coded(item_index, counts, begin, items):
    item_index = (item_index + (items - begin)) & (items - 1)
    low = item_index & (LOW - 1)
    value = jnp.where(low < HALF, low + HALF, -low) << (item_index >> 8)
    position = lax.broadcasted_iota(jnp.int32, item_index.shape, 1)
    return jnp.where(position < counts, value, 0).astype(BF16)


def row_at(y, x, core):
    return (y % SIDE * SIDE + x % SIDE) * CORES + core


def along_col(value, by):
    size = lax.axis_size("col")
    return lax.ppermute(value, "col", [(i, (i + by) % size) for i in range(size)])


def shifted(value, first, by):
    pairs = []
    for y in range(SIDE):
        for x in range(SIDE):
            for core in range(CORES):
                along_x = first == (core == 0)
                to = row_at(y, x + by, core) if along_x else row_at(y + by, x, core)
                pairs.append((row_at(y, x, core), to))
    return lax.ppermute(value, "row", pairs)


def near_of(value, first):
    return shifted(value, first, 1), shifted(value, first, -1)


def far_of(low, high, first):
    return shifted(low, first, 1), shifted(high, first, -1)


def half_sweep(item_factors, item_index, ratings, counts):
    n_row, n_col = lax.axis_size("row"), lax.axis_size("col")
    chips = n_row // CORES
    slots, held = item_index.shape[1], item_factors.shape[0]
    me, z = lax.axis_index("row"), lax.axis_index("col")
    core = me % CORES

    code = coded(item_index, counts, (z + n_col // 2) % n_col * held, n_col * held)
    code = jnp.concatenate([code, ratings], axis=1).reshape(chips, CORES, -1, 2 * slots)
    code = jnp.where(core == 0, code, code[:, ::-1]).reshape(chips, -1, 2 * slots)
    same_core = [[chip * CORES + c for chip in range(chips)] for c in range(CORES)]
    code = lax.all_to_all(code, "row", 0, 0, tiled=True, axis_index_groups=same_core)

    mine = item_factors.T
    three = jnp.stack([along_col(mine, 1), mine, along_col(mine, -1)])
    block = jnp.concatenate([along_col(three, 3), three, along_col(three[:2], -3)])

    who = jnp.full((1,), me, jnp.int32)
    both, own_users, other_users = (0, 1), (0,), (1,)
    half = n_col // 2
    behind, ahead = near_of(block, True)
    alone = block[None]
    alone_behind, alone_ahead = near_of(alone, False)
    far = jnp.concatenate(far_of(behind[:half], ahead[half:], True))[None]
    own, other = gram(who, 0, code, [alone], both)
    sides = jnp.stack([behind, ahead])
    sides_behind, sides_ahead = near_of(sides, False)
    far_behind, far_ahead = near_of(far, False)
    own, other = gram(who, 1, code, [sides, far], both, (own, other))
    low, high = far_of(
        jnp.concatenate([alone_behind, sides_behind[:1]]), jnp.concatenate([sides_ahead[1:], far_ahead]), False
    )
    tables = [alone_behind, sides_behind, far_behind, alone_ahead, sides_ahead, far_ahead]
    own, other = gram(who, 4, code, tables, both, (own, other))
    (other,) = gram(who, 12, code, [low, high], other_users, (other,))
    other = lax.ppermute(other, "row", [(i, i ^ 1) for i in range(n_row)])
    (own,) = gram(who, 12, code, [low, high], own_users, (own,))
    return solve(own, other)[None]


def solution(mesh):
    return jax.shard_map(
        half_sweep,
        mesh=mesh,
        in_specs=(P(("row", "col"), None), P("col", "row"), P("col", "row"), P("col", "row")),
        out_specs=P("col", "row", None),
        check_vma=False,
    )
```

```python
import functools

import jax
import jax.numpy as jnp
from jax import lax
from jax.experimental import pallas as pl
from jax.experimental.pallas import tpu as pltpu
from jax.sharding import PartitionSpec as P


F32, BF16 = jnp.float32, jnp.bfloat16
LOW = 256
HALF = 128
SIDE = 4
CORES = 2
PANEL = 8
BLOCK = 32
VMEM_BYTES = 16 << 20
ROWS_TO_ROWS = (((1,), (1,)), ((), ()))
COLS_TO_COLS = (((0,), (0,)), ((), ()))


def in_vmem(value):
    return pltpu.with_memory_space_constraint(value, pltpu.VMEM)


def chip_of(me, k):
    core, x, y = me & 1, (me >> 1) & (SIDE - 1), me >> 3

    def away(n):
        return jnp.where(n == 1, -1, jnp.where(n == 2, 1, jnp.where(n == 3, 2, 0)))

    first, second = away(k & 3), away(k >> 2)
    dx, dy = jnp.where(core == 0, first, second), jnp.where(core == 0, second, first)
    return ((y + dy) & (SIDE - 1)) * SIDE + ((x + dx) & (SIDE - 1))


def gram_kernel(me_ref, code_ref, *refs, counts, groups, first, offset):
    tables = refs[: len(counts)]
    before = refs[len(counts) : -6 - len(groups)]
    sums = refs[-6 - len(groups) : -6]
    table_s, low_s, high_s, rate_s, live_s, rows_s = refs[-6:]
    users, slots = low_s.shape
    share = users // len(groups)
    rank = sums[0].shape[2]
    step = pl.program_id(0)

    @pl.when(step == 0)
    def _():
        for n, sum_ref in enumerate(sums):
            sum_ref[...] = jnp.zeros(sum_ref.shape, F32) if first else before[n][...]

    begin = 0
    for table_ref, count in zip(tables, counts):

        @pl.when((step >= begin) & (step < begin + count))
        def _(table_ref=table_ref, begin=begin):
            per = LOW // table_ref.shape[3]
            for z in range(table_ref.shape[1]):
                h, q = z // per, z % per
                table_s[h * rank : (h + 1) * rank, q * 128 : (q + 1) * 128] = table_ref[step - begin, z]

        begin += count

    code = code_ref[chip_of(me_ref[0], offset + step)].astype(F32)
    code = jnp.concatenate([code[n * share : (n + 1) * share] for n in groups], axis=0)
    index = code[:, :slots]
    size = jnp.abs(index)
    above = [jnp.where(size >= LOW * 2**e, 1.0, 0.0) for e in range(3)]
    low_s[...] = index * (1.0 - 0.5 * above[0] - 0.25 * above[1] - 0.125 * above[2])
    high_s[...] = above[0] + above[1] + above[2]
    rate_s[...] = code[:, slots:]
    live = jnp.where(size > 0.0, 1.0, 0.0)
    live_s[...] = live[:, : slots // 2] + live[:, slots // 2 :]

    place = lax.broadcasted_iota(jnp.int32, (LOW, slots), 0)
    row_ids = jnp.where(place < HALF, place + HALF, -place).astype(F32).astype(BF16)
    one, zero = jnp.ones((), BF16), jnp.zeros((), BF16)
    table = table_s[...]
    parts = table.shape[0] // rank
    for u in range(users):
        low = jnp.broadcast_to(low_s[u : u + 1], (16, slots)).astype(BF16)
        low = jnp.concatenate([low] * (LOW // 16), axis=0)
        found = jnp.dot(table, jnp.where(row_ids == low, one, zero), preferred_element_type=F32)
        high = jnp.broadcast_to(high_s[u : u + 1], (rank, slots))
        rows = found[:rank]
        for h in range(1, parts):
            rows = jnp.where(high == h, found[h * rank : (h + 1) * rank], rows)
        rows_s[u, :rank] = rows.astype(BF16)
        rows_s[u, rank:] = jnp.broadcast_to(rate_s[u : u + 1], (16, slots)).astype(BF16)
    tail_row = lax.broadcasted_iota(jnp.int32, (8, rank), 0)
    for u in range(users):
        both = rows_s[u]
        out = lax.dot_general(both, both[:rank], ROWS_TO_ROWS, preferred_element_type=F32)
        sum_ref, v = sums[u // share], u % share
        sum_ref[v, :rank] += out[:rank]
        tail = jnp.where(tail_row == 1, jnp.broadcast_to(live_s[u : u + 1], (8, rank)), out[rank : rank + 8])
        sum_ref[v, rank:] += tail


def gram(me, offset, code, tables, groups, before=()):
    _, users, width = code.shape
    slots, share = width // 2, users // CORES
    rank = tables[0].shape[2]
    counts = [t.shape[0] for t in tables]
    users = share * len(groups)
    out = pltpu.VMEM((share, rank + 8, rank), F32)
    whole = pl.BlockSpec(memory_space=pltpu.VMEM)
    operands = [code, *tables, *before]
    pairs = users * sum(counts)
    return pl.pallas_call(
        functools.partial(gram_kernel, counts=counts, groups=groups, first=not before, offset=offset),
        grid_spec=pltpu.PrefetchScalarGridSpec(
            num_scalar_prefetch=1,
            grid=(sum(counts),),
            in_specs=[whole for x in operands],
            out_specs=[whole for n in groups],
            scratch_shapes=[
                pltpu.VMEM((4 * rank, LOW), BF16),
                pltpu.VMEM((users, slots), F32),
                pltpu.VMEM((users, slots), F32),
                pltpu.VMEM((users, slots), F32),
                pltpu.VMEM((users, slots // 2), F32),
                pltpu.VMEM((users, rank + 16, slots), BF16),
            ],
        ),
        out_shape=[out for n in groups],
        cost_estimate=pl.CostEstimate(
            flops=pairs * 2 * slots * (4 * LOW + rank) * rank, transcendentals=0, bytes_accessed=4 * pairs * slots
        ),
        compiler_params=pltpu.CompilerParams(vmem_limit_bytes=VMEM_BYTES),
        name="gram",
    )(me, *[in_vmem(x) for x in operands])


def solve_kernel(own_ref, other_ref, out_ref, rows_s, below_s):
    users, rank = out_ref.shape
    lane = lax.broadcasted_iota(jnp.int32, (users, rank), 1)
    number = jnp.sum(own_ref[:, rank + 1, :] + other_ref[:, rank + 1, :], axis=1, keepdims=True)
    shift = jnp.broadcast_to(0.1 * number / rank, (users, rank))
    for i in range(rank):
        row = own_ref[:, i, :] + other_ref[:, i, :]
        rows_s[i * users : (i + 1) * users] = jnp.where(lane == i, row + shift, row)
    right = own_ref[:, rank, :] + other_ref[:, rank, :]

    def lane_of(value, i):
        return jnp.broadcast_to(value[:, i : i + 1], (users, rank))

    def row_of(i):
        return slice(i * users, (i + 1) * users)

    answer = jnp.zeros((users, rank), F32)
    steps = range(PANEL)
    for top in range(0, rank, BLOCK):
        end = top + BLOCK
        for start in range(top, end, PANEL):
            rows = [rows_s[row_of(start + t)] for t in steps]
            corner = {(t, s): lane_of(rows[s], start + t) for t in steps for s in range(t + 1)}
            middle = [lane_of(right, start + t) for t in steps]
            inside = (lane >= start) & (lane < start + PANEL)
            rows = [jnp.where(inside, jnp.where(lane == start + t, 1.0, 0.0), rows[t]) for t in steps]
            inverse = []
            for s in steps:
                inverse.append(1.0 / corner[s, s])
                for t in range(s + 1, PANEL):
                    factor = corner[t, s] * inverse[s]
                    for q in range(s + 1, t + 1):
                        corner[t, q] = corner[t, q] - factor * corner[q, s]
                    rows[t] = rows[t] - factor * rows[s]
                    middle[t] = middle[t] - factor * middle[s]
            for t in steps:
                scaled = middle[t] * inverse[t]
                answer = answer + jnp.where(lane < start + PANEL, scaled * rows[t], 0.0)
                right = right - scaled * rows[t]
            below = [rows[t] * inverse[t] for t in steps]
            for i in range(start + PANEL, end):
                row = jnp.where(inside, 0.0, rows_s[row_of(i)])
                for t in steps:
                    row = row - lane_of(below[t], i) * rows[t]
                rows_s[row_of(i)] = row
            if end < rank:
                pending = (lane >= start + PANEL) & (lane < end)
                for t in steps:
                    rows_s[row_of(start + t)] = jnp.where(pending, 0.0, rows[t])
                    below_s[row_of(start + t - top)] = below[t]
        if end < rank:
            wide = lax.broadcasted_iota(jnp.int32, (rank - end, rank), 1)
            within = (wide >= top) & (wide < end)
            for u in range(users):
                factors = below_s[pl.ds(u, BLOCK, stride=users), :]
                upper = rows_s[pl.ds(top * users + u, BLOCK, stride=users), :]
                change = lax.dot_general(
                    factors[:, end:],
                    upper,
                    COLS_TO_COLS,
                    precision=lax.Precision.HIGHEST,
                    preferred_element_type=F32,
                )
                rest = pl.ds(end * users + u, rank - end, stride=users)
                rows_s[rest, :] = jnp.where(within, 0.0, rows_s[rest, :]) - change
    out_ref[...] = answer


def solve(own, other):
    users, _, rank = own.shape
    return pl.pallas_call(
        solve_kernel,
        out_shape=jax.ShapeDtypeStruct((users, rank), F32),
        scratch_shapes=[pltpu.VMEM((rank * users, rank), F32), pltpu.VMEM((BLOCK * users, rank), F32)],
        compiler_params=pltpu.CompilerParams(vmem_limit_bytes=VMEM_BYTES),
        name="solve",
    )(in_vmem(own), in_vmem(other))


def coded(item_index, counts, begin, items):
    item_index = (item_index + (items - begin)) & (items - 1)
    low = item_index & (LOW - 1)
    value = jnp.where(low < HALF, low + HALF, -low) << (item_index >> 8)
    position = lax.broadcasted_iota(jnp.int32, item_index.shape, 1)
    return jnp.where(position < counts, value, 0).astype(BF16)


def row_at(y, x, core):
    return (y % SIDE * SIDE + x % SIDE) * CORES + core


def along_col(value, by):
    size = lax.axis_size("col")
    return lax.ppermute(value, "col", [(i, (i + by) % size) for i in range(size)])


def shifted(value, first, by):
    pairs = []
    for y in range(SIDE):
        for x in range(SIDE):
            for core in range(CORES):
                along_x = first == (core == 0)
                to = row_at(y, x + by, core) if along_x else row_at(y + by, x, core)
                pairs.append((row_at(y, x, core), to))
    return lax.ppermute(value, "row", pairs)


def near_of(value, first):
    return shifted(value, first, 1), shifted(value, first, -1)


def far_of(low, high, first):
    return shifted(low, first, 1), shifted(high, first, -1)


def half_sweep(item_factors, item_index, ratings, counts):
    n_row, n_col = lax.axis_size("row"), lax.axis_size("col")
    chips = n_row // CORES
    slots, held = item_index.shape[1], item_factors.shape[0]
    me, z = lax.axis_index("row"), lax.axis_index("col")
    core = me % CORES

    code = coded(item_index, counts, (z + n_col // 2) % n_col * held, n_col * held)
    code = jnp.concatenate([code, ratings], axis=1).reshape(chips, CORES, -1, 2 * slots)
    code = jnp.where(core == 0, code, code[:, ::-1]).reshape(chips, -1, 2 * slots)
    same_core = [[chip * CORES + c for chip in range(chips)] for c in range(CORES)]
    code = lax.all_to_all(code, "row", 0, 0, tiled=True, axis_index_groups=same_core)

    mine = item_factors.T
    three = jnp.stack([along_col(mine, 1), mine, along_col(mine, -1)])
    block = jnp.concatenate([along_col(three, 3), three, along_col(three[:2], -3)])

    who = jnp.full((1,), me, jnp.int32)
    both, own_users, other_users = (0, 1), (0,), (1,)
    half = n_col // 2
    behind, ahead = near_of(block, True)
    three = jnp.stack([block, behind, ahead])
    three_behind, three_ahead = near_of(three, False)
    far = jnp.concatenate(far_of(behind[:half], ahead[half:], True))[None]
    far_behind, far_ahead = near_of(far, False)
    own, other = gram(who, 0, code, [three, far], both)
    low, high = far_of(three_behind[:2], jnp.concatenate([three_ahead[2:], far_ahead]), False)
    tables = [three_behind, far_behind, three_ahead, far_ahead]
    own, other = gram(who, 4, code, tables, both, (own, other))
    (other,) = gram(who, 12, code, [low, high], other_users, (other,))
    other = lax.ppermute(other, "row", [(i, i ^ 1) for i in range(n_row)])
    (own,) = gram(who, 12, code, [low, high], own_users, (own,))
    return solve(own, other)[None]


def solution(mesh):
    return jax.shard_map(
        half_sweep,
        mesh=mesh,
        in_specs=(P(("row", "col"), None), P("col", "row"), P("col", "row"), P("col", "row")),
        out_specs=P("col", "row", None),
        check_vma=False,
    )
```
